32 devices in a mesh: ctx: 8 (over z, core), tp: 4 (over y, x).
Axes of the slice: x: 2, y: 2, z: 4, core: 2. Of those that a mesh axis runs over, the one named last changes fastest.
Arguments:
- tokens: bfloat16 [2, 4096, 8192], P(None, 'ctx', 'tp'), may hold values from -14 to 14
- norm_gain: float32 [8192], replicated, may hold values from 0.5 to 1.5
- span_order: int32 [2, 16], replicated, may hold values from 0 to 15, each once within a row
- w_query: bfloat16 [8192, 4096], P('ctx', 'tp'), may hold values from -0.10122281 to 0.10122281
- w_key: bfloat16 [8192, 1024], P('ctx', 'tp'), may hold values from -0.10122281 to 0.10122281
- value_weight: bfloat16 [8192, 1024], P('ctx', 'tp'), may hold values from -0.0625 to 0.0625
- w_out: bfloat16 [4096, 8192], P('tp', 'ctx'), may hold values from -0.75 to 0.75
Outputs:
- mixed: bfloat16 [2, 4096, 8192], P(None, 'ctx', 'tp')
The draws below stay inside these ranges and needn't reach their ends.
Inputs may be any that keep to these rules, and one draw needn't show every extreme that they name: Each row of span_order names every one of the 2 * 8 blocks of positions once; stored block b of a sequence holds positions span_order[b] * 256 onwards, in order.
All inputs are finite; a program needn't handle non-finite values.
Results may differ from the reference program's by a relative error of at most 0.014.
Values may be sent and summed in bfloat16 or wider, within the bound.
No kernel may reach another device: no remote copies, remote signals or barrier semaphores. Data moves between devices by JAX's collectives and lax.ppermute only.
A program may use at most 128 MiB of HBM per device.

```python
import math
import jax
import jax.numpy as jnp
from jax import lax

MODEL_WIDTH = 8192
QUERY_HEAD_COUNT = 32
KEY_VALUE_HEADS = 8
HEAD_DIM = 128
SEQUENCE_LENGTH = 4096
SEQS = 2
N_CTX = 8
N_TP = 4


def unscaled_weight(key, salt, columns):
    spread = (2.0 / MODEL_WIDTH) ** 0.5
    normal_part = jax.random.normal(jax.random.fold_in(key, salt), (MODEL_WIDTH, columns), jnp.float32)
    return jnp.clip(normal_part, -6.0, 6.0) * spread


def draw_w_query(key, part):
    weight_portion = unscaled_weight(key, 11, QUERY_HEAD_COUNT * HEAD_DIM)
    return weight_portion.astype(jnp.bfloat16)


def draw_w_key(key, part):
    weight_portion = unscaled_weight(key, 12, KEY_VALUE_HEADS * HEAD_DIM)
    return weight_portion.astype(jnp.bfloat16)


def draw_tokens(key, part):
    noise_part = jnp.clip(jax.random.normal(jax.random.fold_in(key, 13), (SEQS, SEQUENCE_LENGTH, MODEL_WIDTH), jnp.float32), -6.0, 6.0)
    return noise_part.astype(jnp.bfloat16)


def level_of(key, extent, cuts, smallest, high):
    loudness = 1.0
    for axis_at, parts in cuts:
        draws = jax.random.uniform(jax.random.fold_in(jax.random.fold_in(key, 6), axis_at), (parts,), jnp.float32, smallest / len(cuts), high / len(cuts))
        loudness = loudness * jnp.repeat(jnp.exp(draws), extent[axis_at] // parts).reshape((-1,) + (1,) * (len(extent) - 1 - axis_at))
    return loudness


def noise(rng, shape, deviation, reach, cuts=(), kind=jnp.bfloat16):
    array = deviation * jax.random.normal(rng, shape, jnp.float32)
    if cuts:
        array = array * level_of(rng, shape, cuts, -0.22, 0.18)
    return jnp.clip(array, -reach, reach).astype(kind)


def setup_inputs(seed: int = 0) -> dict:
    splits = jax.random.split(jax.random.key(seed), 8)
    return {
        "tokens": draw_tokens(jax.random.fold_in(splits[7], 71), 0),
        "norm_gain": jnp.clip(1.0 + 0.1 * jax.random.normal(splits[1], (MODEL_WIDTH,), jnp.float32), 0.5, 1.5),
        "span_order": jax.vmap(lambda own: jax.random.permutation(own, 2 * N_CTX))(jax.random.split(splits[2], SEQS)).reshape((SEQS, 2 * N_CTX)).astype(jnp.int32),
        "w_query": draw_w_query(jax.random.fold_in(splits[7], 71), 0),
        "w_key": draw_w_key(jax.random.fold_in(splits[7], 71), 0),
        "value_weight": noise(splits[5], (MODEL_WIDTH, KEY_VALUE_HEADS * HEAD_DIM), MODEL_WIDTH ** -0.5, 0.0625, ((0, 8), (1, 4))),
        "w_out": noise(splits[6], (QUERY_HEAD_COUNT * HEAD_DIM, MODEL_WIDTH), (QUERY_HEAD_COUNT * HEAD_DIM // 64) ** -0.5, 0.75, ((0, 4), (1, 8))),
    }


theta_base = 500000.0
norm_eps = 1e-05
masked_score = -1e+30

def normalize(flat_rows, norm_gain):
    wide = flat_rows.astype(jnp.float32)
    factor = lax.rsqrt(lax.optimization_barrier(jnp.mean(wide * wide, axis=-1, keepdims=True)) + norm_eps)
    return (wide * factor * norm_gain).astype(jnp.bfloat16)

def positions_of(span_order, first, count, block_rows):
    stored = first + jnp.arange(count, dtype=jnp.int32)
    which = stored // block_rows
    slots = jnp.arange(span_order.shape[1], dtype=jnp.int32)
    picked = lax.optimization_barrier(jnp.sum(jnp.where(slots[None, None, :] == which[None, :, None], span_order[:, None, :], 0), axis=2))
    return (picked * block_rows + stored % block_rows).astype(jnp.int32)

def apply_rotation(value_rows, token_position, head_size):
    half = head_size // 2
    freqs = jnp.exp(-(2.0 * jnp.arange(half, dtype=jnp.float32) / head_size) * math.log(theta_base))
    angle = token_position.astype(jnp.float32)[..., None] * freqs
    cosine = jnp.cos(angle)[:, :, None, :]
    sine = jnp.sin(angle)[:, :, None, :]
    front = value_rows[..., :half]
    back = value_rows[..., half:]
    return jnp.concatenate([front * cosine - back * sine, back * cosine + front * sine], axis=-1)

def reference(tokens, norm_gain, span_order, w_query, w_key, value_weight, w_out):
    sequence_batch = tokens.shape[0]
    token_length = tokens.shape[1]
    block_rows = token_length // (2 * N_CTX)
    normed = normalize(tokens.reshape(sequence_batch * token_length, MODEL_WIDTH), norm_gain)
    token_position = positions_of(span_order, 0, token_length, block_rows)
    query_flat = jnp.dot(normed, w_query, preferred_element_type=jnp.float32)
    flattened_key = jnp.dot(normed, w_key, preferred_element_type=jnp.float32)
    flattened_value = jnp.dot(normed, value_weight, preferred_element_type=jnp.float32)
    query = apply_rotation(query_flat.reshape(sequence_batch, token_length, QUERY_HEAD_COUNT, HEAD_DIM), token_position, HEAD_DIM).astype(jnp.bfloat16)
    key_rows = apply_rotation(flattened_key.reshape(sequence_batch, token_length, KEY_VALUE_HEADS, HEAD_DIM), token_position, HEAD_DIM).astype(jnp.bfloat16)
    value_rows = flattened_value.reshape(sequence_batch, token_length, KEY_VALUE_HEADS, HEAD_DIM).astype(jnp.bfloat16)
    group_width = QUERY_HEAD_COUNT // KEY_VALUE_HEADS
    factor = 1.0 / math.sqrt(HEAD_DIM)
    allowed = token_position[:, None, :] <= token_position[:, :, None]

    def single_head(head):
        query_block = lax.dynamic_slice_in_dim(query, (head * group_width).astype(jnp.int32), group_width, 2).astype(jnp.float32)
        key_block = lax.dynamic_slice_in_dim(key_rows, head.astype(jnp.int32), 1, 2)[:, :, 0, :].astype(jnp.float32)
        value_block = lax.dynamic_slice_in_dim(value_rows, head.astype(jnp.int32), 1, 2)[:, :, 0, :].astype(jnp.float32)
        scores = jnp.einsum('sqgd,skd->sgqk', query_block, key_block) * factor
        scores = jnp.where(allowed[:, None], scores, masked_score)
        peak = lax.optimization_barrier(jnp.max(scores, axis=-1, keepdims=True))
        weights = jnp.where(allowed[:, None], jnp.exp(scores - peak), 0.0)
        total = lax.optimization_barrier(jnp.sum(weights, axis=-1))
        rounded = lax.optimization_barrier(weights.astype(jnp.bfloat16)).astype(jnp.float32)
        summed = jnp.einsum('sgqk,skd->sqgd', rounded, value_block)
        return (summed / jnp.transpose(total, (0, 2, 1))[..., None]).astype(jnp.bfloat16)
    head_outputs = lax.map(single_head, jnp.arange(KEY_VALUE_HEADS, dtype=jnp.int32))
    attended = jnp.transpose(head_outputs, (1, 2, 0, 3, 4)).reshape(sequence_batch * token_length, QUERY_HEAD_COUNT * HEAD_DIM)
    columns = QUERY_HEAD_COUNT * HEAD_DIM // N_TP
    summed = jnp.zeros((sequence_batch * token_length, MODEL_WIDTH), jnp.float32)
    for group in range(N_TP):
        partial_value = jnp.dot(attended[:, group * columns:(group + 1) * columns], w_out[group * columns:(group + 1) * columns], preferred_element_type=jnp.float32)
        summed = summed + lax.optimization_barrier(partial_value.astype(jnp.bfloat16)).astype(jnp.float32)
    return summed.astype(jnp.bfloat16).reshape(sequence_batch, token_length, MODEL_WIDTH)
```

```python
import math

import jax
import jax.numpy as jnp
from jax import lax
from jax.experimental import pallas as pl
from jax.experimental.pallas import tpu as pltpu
from jax.sharding import PartitionSpec as P

HEAD_DIM = 128


theta_base = 500000.0
norm_eps = 1e-05
masked_score = -1e30


def positions_of(span_order, first, count, block_rows):
    stored = first + jnp.arange(count, dtype=jnp.int32)
    which = stored // block_rows
    slots = jnp.arange(span_order.shape[1], dtype=jnp.int32)
    picked = jnp.sum(
        jnp.where(slots[None, None, :] == which[None, :, None], span_order[:, None, :], 0), axis=2
    )
    return picked * block_rows + stored % block_rows


def apply_rotation(value_rows, token_position, head_size):
    half = head_size // 2
    freqs = jnp.exp(-(2.0 * jnp.arange(half, dtype=jnp.float32) / head_size) * math.log(theta_base))
    angle = token_position.astype(jnp.float32)[..., None] * freqs
    cosine = jnp.cos(angle)[:, :, None, :]
    sine = jnp.sin(angle)[:, :, None, :]
    front = value_rows[..., :half]
    back = value_rows[..., half:]
    return jnp.concatenate([front * cosine - back * sine, back * cosine + front * sine], axis=-1)


def attention_kernel(order_ref, place_ref, rank_ref, q_ref, k_ref, v_ref, out_ref, acc_ref, peak_ref, *, block_rows):
    sequence = pl.program_id(0)
    half = pl.program_id(2)
    group_width = q_ref.shape[2]
    head_size = q_ref.shape[4]
    rows = group_width * block_rows
    own_position = order_ref[sequence, rank_ref[0] * 2 + half]
    query = q_ref[0, 0].reshape(rows, head_size)
    scale = math.log2(math.e) / math.sqrt(head_size)
    acc_ref[...] = jnp.zeros_like(acc_ref)
    peak_ref[...] = jnp.full_like(peak_ref, masked_score)

    def step(place, diagonal):
        holder = place // 2
        start = pl.multiple_of((place % 2) * block_rows, block_rows)
        keys = k_ref[holder, 0, 0, pl.ds(start, block_rows), :]
        values = v_ref[holder, 0, 0, pl.ds(start, block_rows), :]
        scores = lax.dot_general(
            query, keys, (((1,), (1,)), ((), ())), preferred_element_type=jnp.float32
        ) * scale
        if diagonal:
            row = lax.broadcasted_iota(jnp.int32, (rows, block_rows), 0) % block_rows
            column = lax.broadcasted_iota(jnp.int32, (rows, block_rows), 1)
            scores = jnp.where(column <= row, scores, masked_score)
        peak = peak_ref[...]
        new_peak = jnp.maximum(peak, jnp.max(scores, axis=1, keepdims=True))
        peak_ref[...] = new_peak
        weights = jnp.exp2(scores - new_peak[:, :1]).astype(jnp.bfloat16)
        shrink = jnp.exp2(peak - new_peak)[:, :1]
        extended = jnp.concatenate([values, jnp.ones_like(values)], axis=1)
        acc_ref[...] = acc_ref[...] * shrink + jnp.dot(
            weights, extended, preferred_element_type=jnp.float32
        )

    step(place_ref[sequence, own_position], True)

    @pl.loop(0, own_position)
    def _(position):
        step(place_ref[sequence, position], False)

    attended = (acc_ref[:, :head_size] / acc_ref[:, head_size:]).astype(out_ref.dtype)
    for head in range(group_width):
        out_ref[0, :, head * head_size : (head + 1) * head_size] = attended[
            head * block_rows : (head + 1) * block_rows
        ]


def attend(span_order, places, rank, query, pairs, block_rows):
    sequences, key_heads, group_width, rows_dev, head_size = query.shape
    holders = pairs.shape[0]
    rows = group_width * block_rows
    return pl.pallas_call(
        lambda *refs: attention_kernel(*refs, block_rows=block_rows),
        out_shape=jax.ShapeDtypeStruct(
            (sequences, rows_dev, key_heads * group_width * head_size), jnp.bfloat16
        ),
        grid_spec=pltpu.PrefetchScalarGridSpec(
            num_scalar_prefetch=3,
            grid=(sequences, key_heads, 2),
            in_specs=[
                pl.BlockSpec(
                    (1, 1, group_width, block_rows, head_size), lambda s, h, b, *_: (s, h, 0, b, 0)
                ),
                pl.BlockSpec(
                    (holders, 1, 1, rows_dev, head_size), lambda s, h, b, *_: (0, s, h, 0, 0)
                ),
                pl.BlockSpec(
                    (holders, 1, 1, rows_dev, head_size),
                    lambda s, h, b, *_: (0, s, h + key_heads, 0, 0),
                ),
            ],
            out_specs=pl.BlockSpec(
                (1, block_rows, group_width * head_size), lambda s, h, b, *_: (s, b, h)
            ),
            scratch_shapes=[
                pltpu.VMEM((rows, 2 * head_size), jnp.float32),
                pltpu.VMEM((rows, 128), jnp.float32),
            ],
        ),
        compiler_params=pltpu.CompilerParams(
            dimension_semantics=("arbitrary", "arbitrary", "arbitrary"),
        ),
        cost_estimate=pl.CostEstimate(
            flops=4 * sequences * rows_dev * holders * rows_dev * key_heads * group_width * head_size,
            bytes_accessed=2 * pairs.size,
            transcendentals=sequences * rows_dev * holders * rows_dev * key_heads * group_width,
        ),
    )(span_order, places, jnp.reshape(rank, (1,)).astype(jnp.int32), query, pairs, pairs)


def per_device(tokens, norm_gain, span_order, w_query, w_key, value_weight, w_out):
    sequence_batch, rows_dev, features = tokens.shape
    head_size = HEAD_DIM
    query_heads = w_query.shape[1] // head_size
    key_heads = w_key.shape[1] // head_size
    group_width = query_heads // key_heads
    block_rows = rows_dev // 2
    total_rows = sequence_batch * rows_dev
    rank = lax.axis_index("ctx")
    mine = lax.axis_index("tp")
    ctx_size = lax.axis_size("ctx")
    tp_size = lax.axis_size("tp")

    def swap(array, bit):
        return lax.ppermute(array, "tp", [(i, i ^ bit) for i in range(tp_size)])

    cut = total_rows // 2
    flat = tokens.reshape(total_rows, features)
    low, high = flat[:cut], flat[cut:]
    if tp_size == 4:
        low_x, high_y = swap(low, 1), swap(high, 2)
        low_y, high_x = swap(low, 2), swap(high, 1)
        low_far, high_far = swap(low_x, 2), swap(high_y, 1)
        pieces = [(low, high), (low_x, high_x), (low_y, high_y), (low_far, high_far)]
    else:
        pieces = [(low, high)] + [(swap(low, i), swap(high, i)) for i in range(1, tp_size)]

    paired = jnp.concatenate([w_key, value_weight], axis=1)
    pair_weight = lax.all_gather(paired, "ctx", axis=0, tiled=True)
    w_query, pair_weight = lax.optimization_barrier((w_query, pair_weight))
    query_weight = lax.all_gather(w_query, "ctx", axis=0, tiled=True)

    def squares(piece):
        wide = piece.astype(jnp.float32)
        return jnp.sum(wide * wide, axis=-1, keepdims=True)

    normed = []
    totals = [sum(squares(piece[side]) for piece in pieces) for side in range(2)]
    factors = [lax.rsqrt(total / (features * tp_size) + norm_eps) for total in totals]
    for bit, piece in enumerate(pieces):
        gain = lax.dynamic_slice_in_dim(norm_gain, (mine ^ bit) * features, features)
        normed.append(
            jnp.concatenate(
                [
                    (piece[side].astype(jnp.float32) * factors[side] * gain).astype(jnp.bfloat16)
                    for side in range(2)
                ],
                axis=0,
            )
        )

    def project(weight):
        out = None
        for bit in range(tp_size):
            rows = lax.dynamic_slice_in_dim(weight, (mine ^ bit) * features, features, 0)
            term = jnp.dot(normed[bit], rows, preferred_element_type=jnp.float32)
            out = term if out is None else out + term
        return out

    query_pos = positions_of(span_order, rank * rows_dev, rows_dev, block_rows)
    both = project(pair_weight)
    key_flat = both[:, : key_heads * head_size]
    value_flat = both[:, key_heads * head_size :]
    own_keys = apply_rotation(
        key_flat.reshape(sequence_batch, rows_dev, key_heads, head_size), query_pos, head_size
    ).astype(jnp.bfloat16)
    own_values = value_flat.reshape(sequence_batch, rows_dev, key_heads, head_size).astype(
        jnp.bfloat16
    )
    own_pairs = jnp.concatenate([own_keys, own_values], axis=2).transpose(0, 2, 1, 3)
    query_weight, own_pairs = lax.optimization_barrier((query_weight, own_pairs))
    pairs = lax.all_gather(own_pairs, "ctx", axis=0)
    query_flat = project(query_weight)
    turned = apply_rotation(
        query_flat.reshape(sequence_batch, rows_dev, query_heads, head_size), query_pos, head_size
    ).astype(jnp.bfloat16)
    query = turned.reshape(sequence_batch, rows_dev, key_heads, group_width, head_size).transpose(
        0, 2, 3, 1, 4
    )

    pairs, w_out = lax.optimization_barrier((pairs, w_out))
    parts = 2
    width = w_out.shape[1] // parts
    out_weights = [
        lax.all_gather(w_out[:, part * width : (part + 1) * width], "ctx", axis=0)
        for part in range(parts)
    ]

    blocks = jnp.arange(span_order.shape[1], dtype=jnp.int32)
    places = jnp.sum(
        jnp.where(span_order[:, :, None] == blocks[None, None, :], blocks[None, :, None], 0), axis=1
    ).astype(jnp.int32)
    attended = attend(span_order, places, rank, query, pairs, block_rows)
    attended = attended.reshape(total_rows, query_heads * head_size)
    sides = (attended[:cut], attended[cut:])
    spread = ctx_size // tp_size

    finished = []
    for weight in out_weights:

        def partial(side, bit):
            columns = lax.dynamic_slice_in_dim(weight, (mine ^ bit) * spread, spread, 0)
            return jnp.stack(
                [
                    jnp.dot(sides[side], columns[i], preferred_element_type=jnp.float32).astype(
                        jnp.bfloat16
                    )
                    for i in range(spread)
                ]
            )

        def wide(array):
            return array.astype(jnp.float32)

        halves = []
        arrived = []
        for side, (first, second) in enumerate(((1, 2), (2, 1))):
            if tp_size != 4:
                terms = [swap(partial(side, bit), bit) for bit in range(1, tp_size)]
                total = sum((wide(term) for term in terms), wide(partial(side, 0)))
                halves.append(total.astype(jnp.bfloat16))
                continue
            near = swap(partial(side, 3), first)
            here = swap(partial(side, first), first)
            arrived += [near, here]
            passing = (wide(partial(side, second)) + wide(near)).astype(jnp.bfloat16)
            far = swap(passing, second)
            halves.append((wide(partial(side, 0)) + wide(here) + wide(far)).astype(jnp.bfloat16))
        finished.append(jnp.concatenate(halves, axis=1))
        sides = lax.optimization_barrier((*sides, *arrived))[:2]
    mixed = jnp.stack(finished, axis=1)
    mixed = mixed.transpose(2, 0, 1, 3)
    return mixed.reshape(sequence_batch, rows_dev, spread * parts * width)


def solution(mesh):
    placed = (
        P(None, "ctx", "tp"),
        P(),
        P(),
        P("ctx", "tp"),
        P("ctx", "tp"),
        P("ctx", "tp"),
        P("tp", "ctx"),
    )
    return jax.shard_map(
        per_device, mesh=mesh, in_specs=placed, out_specs=P(None, "ctx", "tp"), check_vma=False
    )
```
